1024 devices in a mesh: ctx: 128 (over z, y), mp: 8 (over x, core).
Axes of the slice: x: 4, y: 8, z: 16, core: 2. Of those that a mesh axis runs over, the one named last changes fastest.
Arguments:
- queries: bfloat16 [32768, 4096], P('ctx', 'mp'), may hold values from -20 to 20
- keys: bfloat16 [32768, 2048], P('ctx', 'mp'), may hold values from -20 to 20
- values: bfloat16 [32768, 2048], P('ctx', 'mp'), may hold values from -6 to 6
- out_grad: bfloat16 [32768, 4608], P('ctx', 'mp'), may hold values from -6 to 6
- doc_ids: int32 [32768], P('ctx'), may hold values from 0 to 127, never falling along the last dimension, each value on 1 to 768 neighbouring positions
- w_out: bfloat16 [4096, 4608], P('mp'), may hold values from -0.09375 to 0.09375
Outputs:
- query_gradient: bfloat16 [32768, 4096], P('ctx', 'mp')
- key_gradient: bfloat16 [32768, 2048], P('ctx', 'mp')
- value_gradient: bfloat16 [32768, 2048], P('ctx', 'mp')
The draws below stay inside these ranges and needn't reach their ends.
Inputs may be any that keep to these rules, and one draw needn't show every extreme that they name: `doc_ids`: document numbers never fall along the sequence; every document has at most (3) * 256 tokens, and some document has exactly that many.
All inputs are finite; a program needn't handle non-finite values.
Results may differ from the reference program's by a relative error of at most 0.0069.
Values may be sent and summed in bfloat16 or wider, within the bound.
A program may use at most 64 MiB of HBM per device.

```python
import math
import jax
import jax.numpy as jnp
import numpy as np
from jax import lax

D = 4608
QUERY_HEADS = 32
KEY_VALUE_HEADS = 16
HEAD_SIZE = 128
SHARD_TOKENS = 256
SPAN = 4
PACKED_TOKENS = 32768
N_CTX = 128


def shared_parts(key):
    joint_factor = jax.random.fold_in(key, 7100)
    selected_rows = jax.random.randint(jax.random.fold_in(joint_factor, 1), (PACKED_TOKENS, KEY_VALUE_HEADS), 0, 32) == 0
    travel_sense = jax.random.normal(jax.random.fold_in(joint_factor, 2), (KEY_VALUE_HEADS, HEAD_SIZE), jnp.float32)
    travel_sense = travel_sense / jnp.sqrt(jnp.sum(travel_sense * travel_sense, axis=1, keepdims=True))
    return (selected_rows, travel_sense)


def seed_jitter(key, shape):
    return jnp.clip(jax.random.normal(key, shape, jnp.float32), -6.0, 6.0)


def magnitude(key, shape):
    return jnp.exp(jax.random.uniform(key, shape, jnp.float32, jnp.log(17.3), jnp.log(30.0)))


def draw_queries(key, part):
    query_groups = QUERY_HEADS // KEY_VALUE_HEADS
    selected_rows, travel_sense = shared_parts(key)
    local_portion = jax.random.fold_in(key, 7201)
    jitter = seed_jitter(jax.random.fold_in(local_portion, 1), (PACKED_TOKENS, KEY_VALUE_HEADS, query_groups, HEAD_SIZE))
    multiplier = magnitude(jax.random.fold_in(local_portion, 2), (PACKED_TOKENS, KEY_VALUE_HEADS, query_groups))
    multiplier = jnp.where(selected_rows[:, :, None], multiplier, 0.0)
    final_output = jitter + multiplier[..., None] * travel_sense[None, :, None, :]
    return jnp.clip(final_output, -20.0, 20.0).reshape(PACKED_TOKENS, QUERY_HEADS * HEAD_SIZE).astype(jnp.bfloat16)


def draw_keys(key, part):
    selected_rows, travel_sense = shared_parts(key)
    local_portion = jax.random.fold_in(key, 7302)
    jitter = seed_jitter(jax.random.fold_in(local_portion, 1), (PACKED_TOKENS, KEY_VALUE_HEADS, HEAD_SIZE))
    multiplier = magnitude(jax.random.fold_in(local_portion, 2), (PACKED_TOKENS, KEY_VALUE_HEADS))
    multiplier = jnp.where(selected_rows, multiplier, 0.0)
    final_output = jitter + multiplier[..., None] * travel_sense[None, :, :]
    return jnp.clip(final_output, -20.0, 20.0).reshape(PACKED_TOKENS, KEY_VALUE_HEADS * HEAD_SIZE).astype(jnp.bfloat16)


def block_levels(stream_key, extent, split, least, largest):
    def one(dim, blocks):
        heights = jax.random.uniform(jax.random.fold_in(jax.random.fold_in(stream_key, 6), dim), (blocks,), jnp.float32, least / len(split), largest / len(split))
        return jnp.repeat(jnp.exp(heights), extent[dim] // blocks).reshape((-1,) + (1,) * (len(extent) - dim - 1))

    loudness = one(*split[0])
    for cut in split[1:]:
        loudness = loudness * one(*cut)
    return loudness


def profile(amount, total, reach, slope):
    loads = [(1 << 20) // math.isqrt(rank ** slope) + 1 for rank in range(2, amount + 1)]
    spare, given = total - reach - (amount - 1), [1] * (amount - 1)
    while spare > 0:
        candidates = [i for i in range(amount - 1) if given[i] < reach]
        pool, remaining = sum([loads[i] for i in candidates]), spare
        for i in candidates:
            addition = min(reach - given[i], max(1, remaining * loads[i] // pool), spare)
            given[i] = given[i] + addition
            spare = spare - addition
    return np.array([reach] + given)


def uneven_parts(own_key, amount, total, bound, lean):
    if amount == 2:
        one = jax.random.randint(own_key, (), max(1, total - bound), min(bound, total - 1) + 1)
        return jnp.stack([one, total - one])
    tallies = jnp.asarray(profile(amount, total, bound, lean), jnp.int32)
    pairs = (amount - 1) // 2
    source_of, sink = tallies[1:1 + 2 * pairs:2], tallies[2:2 + 2 * pairs:2]
    room = jnp.minimum(source_of - 1, bound - sink)
    shifted = jax.random.randint(jax.random.fold_in(own_key, 1), (pairs,), 0, 1 << 20) % (room + 1)
    tallies = tallies.at[1:1 + 2 * pairs:2].set(source_of - shifted).at[2:2 + 2 * pairs:2].set(sink + shifted)
    return tallies[jax.random.permutation(jax.random.fold_in(own_key, 2), amount)]


def gaussian(key, extent, scale, limit, cuts=(), kind=jnp.bfloat16):
    loudness = block_levels(key, extent, cuts, -0.22, 0.18) if cuts else 1.0
    entries = jax.random.normal(key, extent, jnp.float32) * scale * loudness
    return jnp.minimum(jnp.maximum(entries, -limit), limit).astype(kind)


def setup_inputs(seed: int = 0) -> dict:
    key_of = jax.random.split(jax.random.key(seed), 7)
    queries = draw_queries(jax.random.fold_in(key_of[6], 71), 0)
    keys = draw_keys(jax.random.fold_in(key_of[6], 71), 0)
    values = gaussian(key_of[2], (PACKED_TOKENS, KEY_VALUE_HEADS * HEAD_SIZE), 1.0, 6.0, ((0, 128), (1, 8)))
    out_grad = gaussian(key_of[3], (PACKED_TOKENS, D), 1.0, 6.0, ((0, 128), (1, 8)))
    doc_ids = jnp.searchsorted(jnp.cumsum(uneven_parts(key_of[4], N_CTX, PACKED_TOKENS, (SPAN - 1) * SHARD_TOKENS, 2)), jnp.arange(PACKED_TOKENS), side="right").astype(jnp.int32)
    w_out = gaussian(key_of[5], (QUERY_HEADS * HEAD_SIZE, D), D ** -0.5, 0.09375, ((0, 8),))
    return {"queries": queries, "keys": keys, "values": values, "out_grad": out_grad, "doc_ids": doc_ids, "w_out": w_out}


cap_value = 50.0
query_scale = 1.0 / 12.0


def tile_scores(query_quad, key_slab):
    raw = jnp.einsum("qhgd,khd->hgqk", query_quad.astype(jnp.float32), key_slab.astype(jnp.float32))
    tanh_part = jnp.tanh(raw * (query_scale / cap_value))
    return cap_value * tanh_part, tanh_part


def reference(queries, keys, values, out_grad, doc_ids, w_out):
    query_groups = QUERY_HEADS // KEY_VALUE_HEADS
    visible_span = SPAN * SHARD_TOKENS
    leading_edge = (SPAN - 1) * SHARD_TOKENS
    padded_keys = jnp.concatenate([jnp.zeros((leading_edge, KEY_VALUE_HEADS * HEAD_SIZE), jnp.bfloat16), keys])
    padded_values = jnp.concatenate([jnp.zeros((leading_edge, KEY_VALUE_HEADS * HEAD_SIZE), jnp.bfloat16), values])
    ids_front = jnp.concatenate([jnp.full((leading_edge,), -1, jnp.int32), doc_ids])
    offsets = jnp.arange(SHARD_TOKENS, dtype=jnp.int32)
    spots = jnp.arange(visible_span, dtype=jnp.int32)
    weight_full = w_out.astype(jnp.float32)

    def query_block(index):
        span_opening = (index * SHARD_TOKENS).astype(jnp.int32)
        query_quad = lax.dynamic_slice_in_dim(queries, span_opening, SHARD_TOKENS, 0).reshape(SHARD_TOKENS, KEY_VALUE_HEADS, query_groups, HEAD_SIZE)
        grad_rows = lax.dynamic_slice_in_dim(out_grad, span_opening, SHARD_TOKENS, 0).astype(jnp.float32)
        incoming_gradient = lax.dot_general(grad_rows, weight_full, (((1,), (1,)), ((), ()))).astype(jnp.bfloat16)
        gradient_quad = incoming_gradient.reshape(SHARD_TOKENS, KEY_VALUE_HEADS, query_groups, HEAD_SIZE)
        key_slab = lax.dynamic_slice_in_dim(padded_keys, span_opening, visible_span, 0).reshape(visible_span, KEY_VALUE_HEADS, HEAD_SIZE)
        value_slab = lax.dynamic_slice_in_dim(padded_values, span_opening, visible_span, 0).reshape(visible_span, KEY_VALUE_HEADS, HEAD_SIZE)
        key_ids = lax.dynamic_slice_in_dim(ids_front, span_opening, visible_span, 0)
        query_ids = lax.dynamic_slice_in_dim(doc_ids, span_opening, SHARD_TOKENS, 0)
        key_pos = span_opening - leading_edge + spots
        query_pos = span_opening + offsets
        mask = (query_ids[:, None] == key_ids[None, :]) & (key_pos[None, :] <= query_pos[:, None])
        scores, tanh_part = tile_scores(query_quad, key_slab)
        weights = jnp.where(mask, jnp.exp(scores), 0.0)
        total = jnp.sum(weights, axis=3)
        logsum_total = jnp.log(total)
        value_sum = jnp.einsum("hgqk,khd->qhgd", weights.astype(jnp.bfloat16).astype(jnp.float32), value_slab.astype(jnp.float32))
        attended = value_sum / jnp.transpose(total, (2, 0, 1))[..., None]
        row_correction = jnp.transpose(jnp.sum(gradient_quad.astype(jnp.float32) * attended, axis=3), (1, 2, 0))
        probs = jnp.where(mask, jnp.exp(scores - logsum_total[..., None]), 0.0)
        prob_grad = jnp.einsum("qhgd,khd->hgqk", gradient_quad.astype(jnp.float32), value_slab.astype(jnp.float32))
        logit_grad = (probs * (prob_grad - row_correction[..., None]) * (1.0 - tanh_part * tanh_part) * query_scale).astype(jnp.bfloat16)
        query_part = jnp.einsum("hgqk,khd->qhgd", logit_grad.astype(jnp.float32), key_slab.astype(jnp.float32))
        return (query_part.reshape(SHARD_TOKENS, QUERY_HEADS * HEAD_SIZE).astype(jnp.bfloat16), incoming_gradient,
                jnp.transpose(logsum_total, (2, 0, 1)), jnp.transpose(row_correction, (2, 0, 1)))

    query_gradient, incoming_gradient, logsum_total, row_correction = lax.map(query_block, jnp.arange(N_CTX, dtype=jnp.int32))
    query_gradient = query_gradient.reshape(PACKED_TOKENS, QUERY_HEADS * HEAD_SIZE)
    padded_gradient = jnp.concatenate([incoming_gradient.reshape(PACKED_TOKENS, QUERY_HEADS * HEAD_SIZE), jnp.zeros((leading_edge, QUERY_HEADS * HEAD_SIZE), jnp.bfloat16)])
    padded_queries = jnp.concatenate([queries, jnp.zeros((leading_edge, QUERY_HEADS * HEAD_SIZE), jnp.bfloat16)])
    ids_back = jnp.concatenate([doc_ids, jnp.full((leading_edge,), -1, jnp.int32)])
    padded_logsum = jnp.concatenate([logsum_total.reshape(PACKED_TOKENS, KEY_VALUE_HEADS, query_groups), jnp.zeros((leading_edge, KEY_VALUE_HEADS, query_groups), jnp.float32)])
    padded_correction = jnp.concatenate([row_correction.reshape(PACKED_TOKENS, KEY_VALUE_HEADS, query_groups), jnp.zeros((leading_edge, KEY_VALUE_HEADS, query_groups), jnp.float32)])

    def key_block_grads(index):
        span_opening = (index * SHARD_TOKENS).astype(jnp.int32)
        key_slab = lax.dynamic_slice_in_dim(keys, span_opening, SHARD_TOKENS, 0).reshape(SHARD_TOKENS, KEY_VALUE_HEADS, HEAD_SIZE)
        value_slab = lax.dynamic_slice_in_dim(values, span_opening, SHARD_TOKENS, 0).reshape(SHARD_TOKENS, KEY_VALUE_HEADS, HEAD_SIZE)
        key_ids = lax.dynamic_slice_in_dim(doc_ids, span_opening, SHARD_TOKENS, 0)
        query_quad = lax.dynamic_slice_in_dim(padded_queries, span_opening, visible_span, 0).reshape(visible_span, KEY_VALUE_HEADS, query_groups, HEAD_SIZE)
        gradient_quad = lax.dynamic_slice_in_dim(padded_gradient, span_opening, visible_span, 0).reshape(visible_span, KEY_VALUE_HEADS, query_groups, HEAD_SIZE)
        query_ids = lax.dynamic_slice_in_dim(ids_back, span_opening, visible_span, 0)
        log_rows = jnp.transpose(lax.dynamic_slice_in_dim(padded_logsum, span_opening, visible_span, 0), (1, 2, 0))
        delta_rows = jnp.transpose(lax.dynamic_slice_in_dim(padded_correction, span_opening, visible_span, 0), (1, 2, 0))
        key_pos = span_opening + offsets
        query_pos = span_opening + spots
        mask = (query_ids[:, None] == key_ids[None, :]) & (key_pos[None, :] <= query_pos[:, None])
        scores, tanh_part = tile_scores(query_quad, key_slab)
        probs = jnp.where(mask, jnp.exp(scores - log_rows[..., None]), 0.0)
        prob_grad = jnp.einsum("qhgd,khd->hgqk", gradient_quad.astype(jnp.float32), value_slab.astype(jnp.float32))
        logit_grad = (probs * (prob_grad - delta_rows[..., None]) * (1.0 - tanh_part * tanh_part) * query_scale).astype(jnp.bfloat16)
        key_portion = jnp.einsum("hgqk,qhgd->khd", logit_grad.astype(jnp.float32), query_quad.astype(jnp.float32))
        value_portion = jnp.einsum("hgqk,qhgd->khd", probs.astype(jnp.bfloat16).astype(jnp.float32), gradient_quad.astype(jnp.float32))
        return (key_portion.reshape(SHARD_TOKENS, KEY_VALUE_HEADS * HEAD_SIZE).astype(jnp.bfloat16),
                value_portion.reshape(SHARD_TOKENS, KEY_VALUE_HEADS * HEAD_SIZE).astype(jnp.bfloat16))

    key_gradient, value_gradient = lax.map(key_block_grads, jnp.arange(N_CTX, dtype=jnp.int32))
    return query_gradient, key_gradient.reshape(PACKED_TOKENS, KEY_VALUE_HEADS * HEAD_SIZE), value_gradient.reshape(PACKED_TOKENS, KEY_VALUE_HEADS * HEAD_SIZE)
```

```python
import functools
import jax
import jax.numpy as jnp
from jax import lax
from jax.experimental import pallas as pl
from jax.experimental.pallas import tpu as pltpu
from jax.sharding import PartitionSpec as P

HEAD = 128
SPAN = 4
GROUP = 2
CAP = 50.0
SCALE = 1.0 / 12.0
MESH = pl.DeviceIdType.MESH
BF = jnp.bfloat16
F32 = jnp.float32
CHIPS = 4


def lanes_dot(a, b):
    return lax.dot_general(a, b, (((1,), (1,)), ((), ())), preferred_element_type=F32)


def rows_dot(a, b):
    return lax.dot_general(a, b, (((0,), (0,)), ((), ())), preferred_element_type=F32)


def plain_dot(a, b):
    return lax.dot_general(a, b, (((1,), (0,)), ((), ())), preferred_element_type=F32)


def fold_rows(a):
    rows, cols = a.shape
    return jnp.sum(a.reshape(rows // 8, 8, cols), axis=0)


def kernel(
    n_ctx, rows,
    q_hbm, k_hbm, v_hbm, og_hbm, ids_hbm, w_hbm,
    dq_ref, dk_ref, dv_ref,
    q_v, kbuf, vbuf, ogbuf, idbuf, w_v, do_v,
    cb, wb, lacc, att, dqt, gacc, kid, snd, rcv,
    load_sem, kv_s, kv_r, id_s, id_r, x_s, x_r, b_s, b_r,
):
    here = lax.axis_index("ctx")
    m = lax.axis_index("mp")
    x = m // 2
    c = m % 2
    nxt = lax.rem(here + 1, n_ctx)
    prv = lax.rem(here + n_ctx - 1, n_ctx)
    partner = x * 2 + (1 - c)
    right = lax.rem(x + 1, CHIPS) * 2 + c
    left = lax.rem(x + CHIPS - 1, CHIPS) * 2 + c
    deep = ogbuf.shape[2]
    half = deep // 2
    top, bot = pl.ds(0, half), pl.ds(half, half)
    pair = w_hbm.shape[1] // CHIPS
    has_next = here < n_ctx - 1
    has_prev = here > 0

    loads = {}

    def load(name, src, dst):
        cp = pltpu.make_async_copy(src, dst, load_sem.at[len(loads)])
        cp.start()
        loads[name] = cp

    for g in range(2):
        cols = pl.ds(g * HEAD, HEAD)
        load(("k", g), k_hbm.at[:, cols], kbuf.at[0, g])
        load(("v", g), v_hbm.at[:, cols], vbuf.at[0, g])
        if g == 0:
            load("og", og_hbm, ogbuf.at[0, c])
            load("ids", ids_hbm, idbuf.at[0])
            load("q", q_hbm, q_v)
    load("w", w_hbm, w_v)

    barrier = pltpu.get_barrier_semaphore()
    for peer in ({"mp": partner}, {"mp": right}, {"mp": left}):
        pl.semaphore_signal(barrier, inc=1, device_id=peer, device_id_type=MESH)

    @pl.when(has_next)
    def _():
        pl.semaphore_signal(barrier, inc=1, device_id={"ctx": nxt}, device_id_type=MESH)

    @pl.when(has_prev)
    def _():
        pl.semaphore_signal(barrier, inc=1, device_id={"ctx": prv}, device_id_type=MESH)

    @pl.when(here == 0)
    def _():
        kbuf[1:] = jnp.zeros((SPAN - 1, *kbuf.shape[1:]), BF)
        vbuf[1:] = jnp.zeros((SPAN - 1, *vbuf.shape[1:]), BF)
        idbuf[1:] = jnp.zeros((SPAN - 1, *idbuf.shape[1:]), jnp.int32)

    @pl.when(here == n_ctx - 1)
    def _():
        rcv[...] = jnp.zeros(rcv.shape, BF)

    pl.semaphore_wait(barrier, 3 + has_next.astype(jnp.int32) + has_prev.astype(jnp.int32))

    def remote(src, dst, ssem, rsem, peer):
        return pltpu.make_async_remote_copy(
            src_ref=src, dst_ref=dst, send_sem=ssem, recv_sem=rsem,
            device_id=peer, device_id_type=MESH,
        )

    def kv_copy(hop, g, which):
        buf = kbuf if which == 0 else vbuf
        return remote(buf.at[hop, g], buf.at[hop + 1, g], kv_s.at[hop, g, which],
                      kv_r.at[hop, g, which], {"ctx": nxt})

    def id_copy(hop):
        return remote(idbuf.at[hop], idbuf.at[hop + 1], id_s.at[hop], id_r.at[hop], {"ctx": nxt})

    def og_copy(i, src_slot, dst_slot, part, peer):
        return remote(ogbuf.at[src_slot, c, part], ogbuf.at[dst_slot, c, part],
                      x_s.at[i], x_r.at[i], {"mp": peer})

    started = []

    def go(cp, when=None):
        if when is None:
            cp.start()
        else:
            pl.when(when)(lambda: cp.start())
        started.append((cp, when))

    def arrive(cp, when):
        pl.when(when)(lambda: cp.wait_recv())

    kv = {(hop, g, w): kv_copy(hop, g, w) for hop in range(3) for g in range(2) for w in range(2)}
    idc = [id_copy(hop) for hop in range(3)]
    everything = pl.ds(0, deep)
    og_own = og_copy(0, 0, 0, everything, partner)
    og_rt = og_copy(1, 0, 1, top, right)
    og_rb = og_copy(2, 0, 1, bot, right)
    og_lb = og_copy(3, 0, 3, bot, left)
    og_lt = og_copy(4, 0, 3, top, left)
    og_fr = og_copy(5, 1, 2, top, right)
    og_fl = og_copy(6, 3, 2, bot, left)
    share = {
        (1, 0): og_copy(7, 1, 1, top, partner),
        (1, 1): og_copy(8, 1, 1, bot, partner),
        (3, 0): og_copy(9, 3, 3, top, partner),
        (3, 1): og_copy(10, 3, 3, bot, partner),
        (2, 0): og_copy(11, 2, 2, top, partner),
        (2, 1): og_copy(12, 2, 2, bot, partner),
    }

    loads[("k", 0)].wait()
    go(kv[0, 0, 0], has_next)
    loads["og"].wait()
    go(og_rt)
    go(og_lb)
    go(og_rb)
    go(og_lt)
    go(og_own)
    loads[("v", 0)].wait()
    loads["ids"].wait()
    go(idc[0], has_next)
    go(kv[0, 0, 1], has_next)

    def forward(hop, g, which):
        arrive(kv[hop - 1, g, which], has_prev)
        if hop < 3:
            go(kv[hop, g, which], has_next)

    def spread_ids(hop):
        row = idbuf[hop]
        if hop:
            row = jnp.where(here >= hop, row, -1)
        kid[hop] = jnp.transpose(jnp.broadcast_to(row, (HEAD, rows)))

    def score(g, hop):
        keys = kbuf[hop, g]
        visible = jnp.concatenate([kid[hop]] * (rows // HEAD), axis=1) == jnp.broadcast_to(idbuf[0], (rows, rows))
        if hop == 0:
            visible = visible & (
                lax.broadcasted_iota(jnp.int32, (rows, rows), 0)
                <= lax.broadcasted_iota(jnp.int32, (rows, rows), 1)
            )
        for h in range(GROUP):
            i = g * GROUP + h
            t = jnp.tanh(lanes_dot(keys, q_v[:, i * HEAD:(i + 1) * HEAD]) * (SCALE / CAP))
            w = jnp.where(visible, jnp.exp(CAP * t), 0.0)
            wb[hop, i] = w
            cb[hop, i] = w * (SCALE - SCALE * (t * t))
            part = fold_rows(w)
            lacc[i] = part if hop == 0 else lacc[i] + part

    def attend(g, hop):
        vals = vbuf[hop, g]
        for h in range(GROUP):
            i = g * GROUP + h
            part = rows_dot(vals, wb[hop, i].astype(BF))
            att[i] = part if hop == 0 else att[i] + part

    def inverse(g):
        return [1.0 / jnp.sum(lacc[g * GROUP + h], axis=0, keepdims=True) for h in range(GROUP)]

    def deltas(g, inv):
        out = []
        for h in range(GROUP):
            i = g * GROUP + h
            d = do_v[i * HEAD:(i + 1) * HEAD, :].astype(F32)
            out.append(jnp.sum(d * att[i], axis=0, keepdims=True) * inv[h])
        return out

    def back_v(g, hop, inv):
        total = None
        for h in range(GROUP):
            i = g * GROUP + h
            probs = (wb[hop, i] * inv[h]).astype(BF)
            part = lanes_dot(probs, do_v[i * HEAD:(i + 1) * HEAD, :])
            total = part if total is None else total + part
        return total

    def back_k(g, hop, inv, delta):
        keys, vals = kbuf[hop, g], vbuf[hop, g]
        total = None
        for h in range(GROUP):
            i = g * GROUP + h
            grad = plain_dot(vals, do_v[i * HEAD:(i + 1) * HEAD, :])
            slope = ((cb[hop, i] * inv[h]) * (grad - delta[h])).astype(BF)
            part = plain_dot(slope, q_v[:, i * HEAD:(i + 1) * HEAD])
            total = part if total is None else total + part
            d = rows_dot(keys, slope)
            dqt[i] = d if hop == 3 else dqt[i] + d
        return total

    def back_copy(step, g, which):
        return remote(snd.at[step, g, which], rcv.at[step, g, which], b_s.at[step, g, which],
                      b_r.at[step, g, which], {"ctx": prv})

    bc = {(s, g, w): back_copy(s, g, w) for s in range(3) for g in range(2) for w in range(2)}

    def project(rel):
        at = pl.multiple_of(lax.rem(x + CHIPS - rel, CHIPS) * pair, HEAD)
        part = plain_dot(w_v[:, pl.ds(at, pair)], ogbuf[rel].reshape(pair, rows))
        if rel == 0:
            gacc[...] = part
        elif rel == 2:
            do_v[...] = (gacc[...] + part).astype(BF)
        else:
            gacc[...] += part

    def pass_on(g, hop, which, value):
        step = 3 - hop
        if step:
            arrive(bc[step - 1, g, which], has_next)
            value = value + rcv[step - 1, g, which].astype(F32)
        if hop:
            snd[step, g, which] = value.astype(BF)
            go(bc[step, g, which], has_prev)
        else:
            out = dk_ref if which == 0 else dv_ref
            out[:, g * HEAD:(g + 1) * HEAD] = value.astype(BF)

    def begin(g, hop, inv, delta):
        dv = back_v(g, hop, inv)
        dk = back_k(g, hop, inv, delta) if hop < 3 else None
        pass_on(g, hop, 1, dv)
        if dk is None:
            dk = back_k(g, hop, inv, delta)
        pass_on(g, hop, 0, dk)

    def emit_q(g):
        for h in range(GROUP):
            i = g * GROUP + h
            dq_ref[:, i * HEAD:(i + 1) * HEAD] = jnp.transpose(dqt[i]).astype(BF)

    def ids_forward(hop):
        arrive(idc[hop - 1], has_prev)
        if hop < 3:
            go(idc[hop], has_next)
        spread_ids(hop)

    loads["q"].wait()
    loads[("k", 1)].wait()
    loads[("v", 1)].wait()
    spread_ids(0)
    score(0, 0)
    attend(0, 0)
    forward(1, 0, 0)
    og_own.wait_recv()
    loads["w"].wait()
    ids_forward(1)
    score(0, 1)
    forward(1, 0, 1)
    attend(0, 1)
    project(0)
    og_rt.wait_recv()
    go(og_fr)
    go(share[1, 0])
    og_lb.wait_recv()
    go(og_fl)
    go(share[3, 1])
    forward(2, 0, 0)
    ids_forward(2)
    score(0, 2)
    forward(2, 0, 1)
    go(kv[0, 1, 0], has_next)
    go(kv[0, 1, 1], has_next)
    attend(0, 2)
    score(1, 0)
    attend(1, 0)
    og_rb.wait_recv()
    go(share[1, 1])
    og_lt.wait_recv()
    go(share[3, 0])
    forward(3, 0, 0)
    ids_forward(3)
    score(0, 3)
    share[1, 0].wait_recv()
    share[1, 1].wait_recv()
    project(1)
    forward(3, 0, 1)
    attend(0, 3)
    inv_a = inverse(0)
    share[3, 0].wait_recv()
    share[3, 1].wait_recv()
    project(3)
    forward(1, 1, 0)
    og_fr.wait_recv()
    go(share[2, 0])
    og_fl.wait_recv()
    go(share[2, 1])
    score(1, 1)
    forward(1, 1, 1)
    share[2, 0].wait_recv()
    share[2, 1].wait_recv()
    project(2)
    delta_a = deltas(0, inv_a)
    begin(0, 3, inv_a, delta_a)
    attend(1, 1)
    forward(2, 1, 0)
    score(1, 2)
    forward(2, 1, 1)
    attend(1, 2)
    begin(0, 2, inv_a, delta_a)
    forward(3, 1, 0)
    score(1, 3)
    inv_b = inverse(1)
    pass_on(1, 3, 1, back_v(1, 3, inv_b))
    forward(3, 1, 1)
    attend(1, 3)
    delta_b = deltas(1, inv_b)
    pass_on(1, 3, 0, back_k(1, 3, inv_b, delta_b))
    begin(0, 1, inv_a, delta_a)
    begin(1, 2, inv_b, delta_b)
    begin(0, 0, inv_a, delta_a)
    emit_q(0)
    begin(1, 1, inv_b, delta_b)
    begin(1, 0, inv_b, delta_b)
    emit_q(1)
    for cp, when in started:
        if when is None:
            cp.wait_send()
        else:
            pl.when(when)(functools.partial(cp.wait_send))


def settle(*refs):
    sems = refs[-1]
    n = len(refs) // 2
    copies = [pltpu.make_async_copy(refs[i], refs[n + i], sems.at[i]) for i in range(n)]
    for cp in copies:
        cp.start()
    for cp in copies:
        cp.wait()


def body(n_ctx, queries, keys, values, out_grad, doc_ids, w_out):
    rows = queries.shape[0]
    heads = queries.shape[1] // HEAD
    dma = pltpu.SemaphoreType.DMA
    anywhere = pl.BlockSpec(memory_space=pl.ANY)
    vmem = pl.BlockSpec(memory_space=pltpu.VMEM)
    shapes = (queries.shape, keys.shape, values.shape)
    grads = pl.pallas_call(
        functools.partial(kernel, n_ctx, rows),
        out_shape=tuple(pltpu.VMEM(sh, BF) for sh in shapes),
        in_specs=[anywhere] * 6,
        out_specs=(vmem, vmem, vmem),
        scratch_shapes=[
            pltpu.VMEM(queries.shape, BF),
            pltpu.VMEM((SPAN, 2, rows, HEAD), BF),
            pltpu.VMEM((SPAN, 2, rows, HEAD), BF),
            pltpu.VMEM((CHIPS, 2, out_grad.shape[1], rows), BF),
            pltpu.VMEM((SPAN, 1, rows), jnp.int32),
            pltpu.VMEM(w_out.shape, BF),
            pltpu.VMEM((heads * HEAD, rows), BF),
            pltpu.VMEM((SPAN, heads, rows, rows), F32),
            pltpu.VMEM((SPAN, heads, rows, rows), F32),
            pltpu.VMEM((heads, 8, rows), F32),
            pltpu.VMEM((heads, HEAD, rows), F32),
            pltpu.VMEM((heads, HEAD, rows), F32),
            pltpu.VMEM((heads * HEAD, rows), F32),
            pltpu.VMEM((SPAN, rows, HEAD), jnp.int32),
            pltpu.VMEM((3, 2, 2, rows, HEAD), BF),
            pltpu.VMEM((3, 2, 2, rows, HEAD), BF),
            dma((8,)),
            dma((3, 2, 2)),
            dma((3, 2, 2)),
            dma((3,)),
            dma((3,)),
            dma((13,)),
            dma((13,)),
            dma((3, 2, 2)),
            dma((3, 2, 2)),
        ],
        compiler_params=pltpu.CompilerParams(
            collective_id=0, has_side_effects=True, vmem_limit_bytes=60000 * 1024
        ),
    )(queries, keys, values, out_grad.T, doc_ids.reshape(1, rows), w_out)
    grads = [pltpu.with_memory_space_constraint(g, pltpu.VMEM) for g in grads]
    return pl.pallas_call(
        settle,
        out_shape=tuple(jax.ShapeDtypeStruct(sh, BF) for sh in shapes),
        in_specs=[vmem] * 3,
        out_specs=(anywhere,) * 3,
        scratch_shapes=[dma((3,))],
    )(*grads)


def solution(mesh):
    placed = (
        P("ctx", "mp"),
        P("ctx", "mp"),
        P("ctx", "mp"),
        P("ctx", "mp"),
        P("ctx"),
        P("mp", None),
    )
    return jax.shard_map(
        functools.partial(body, mesh.shape["ctx"]),
        mesh=mesh,
        in_specs=placed,
        out_specs=(P("ctx", "mp"), P("ctx", "mp"), P("ctx", "mp")),
        check_vma=False,
    )
```

```python
import functools
import jax
import jax.numpy as jnp
from jax import lax
from jax.experimental import pallas as pl
from jax.experimental.pallas import tpu as pltpu
from jax.sharding import PartitionSpec as P

HEAD = 128
SPAN = 4
GROUP = 2
CAP = 50.0
SCALE = 1.0 / 12.0
MESH = pl.DeviceIdType.MESH
BF = jnp.bfloat16
F32 = jnp.float32
CHIPS = 4
PIECES = 2


def lanes_dot(a, b):
    return lax.dot_general(a, b, (((1,), (1,)), ((), ())), preferred_element_type=F32)


def rows_dot(a, b):
    return lax.dot_general(a, b, (((0,), (0,)), ((), ())), preferred_element_type=F32)


def plain_dot(a, b):
    return lax.dot_general(a, b, (((1,), (0,)), ((), ())), preferred_element_type=F32)


def fold_rows(a):
    rows, cols = a.shape
    return jnp.sum(a.reshape(rows // 8, 8, cols), axis=0)


def kernel(
    n_ctx, rows,
    q_hbm, k_hbm, v_hbm, og_hbm, ids_hbm, w_hbm,
    dq_ref, dk_ref, dv_ref,
    q_v, kbuf, vbuf, ogbuf, idbuf, w_v, do_v,
    cb, wb, lacc, att, dqt, gacc, kid, part, snd, rcv,
    load_sem, kv_s, kv_r, id_s, id_r, x_s, x_r, b_s, b_r,
):
    here = lax.axis_index("ctx")
    m = lax.axis_index("mp")
    x = m // 2
    c = m % 2
    nxt = lax.rem(here + 1, n_ctx)
    prv = lax.rem(here + n_ctx - 1, n_ctx)
    partner = x * 2 + (1 - c)
    right = lax.rem(x + 1, CHIPS) * 2 + c
    left = lax.rem(x + CHIPS - 1, CHIPS) * 2 + c
    deep = ogbuf.shape[2]
    half = deep // 2
    top, bot = pl.ds(0, half), pl.ds(half, half)
    pair = w_hbm.shape[1] // CHIPS
    has_next = here < n_ctx - 1
    has_prev = here > 0
    pieces = [pl.ds(n * (rows // PIECES), rows // PIECES) for n in range(PIECES)]

    barrier = pltpu.get_barrier_semaphore()
    for peer in ({"mp": partner}, {"mp": right}, {"mp": left}):
        pl.semaphore_signal(barrier, inc=1, device_id=peer, device_id_type=MESH)

    @pl.when(has_next)
    def _():
        pl.semaphore_signal(barrier, inc=1, device_id={"ctx": nxt}, device_id_type=MESH)

    @pl.when(has_prev)
    def _():
        pl.semaphore_signal(barrier, inc=1, device_id={"ctx": prv}, device_id_type=MESH)

    loads = {}

    def load(name, src, dst):
        cp = pltpu.make_async_copy(src, dst, load_sem.at[len(loads)])
        cp.start()
        loads[name] = cp

    for g in range(2):
        cols = pl.ds(g * HEAD, HEAD)
        load(("k", g), k_hbm.at[:, cols], kbuf.at[0, g])
        load(("v", g), v_hbm.at[:, cols], vbuf.at[0, g])
        if g == 0:
            load("og", og_hbm, ogbuf.at[0, c])
            load("ids", ids_hbm, idbuf.at[0])
            load("q", q_hbm, q_v)
    load("w", w_hbm, w_v)

    @pl.when(here == 0)
    def _():
        kbuf[1:] = jnp.zeros((SPAN - 1, *kbuf.shape[1:]), BF)
        vbuf[1:] = jnp.zeros((SPAN - 1, *vbuf.shape[1:]), BF)
        idbuf[1:] = jnp.zeros((SPAN - 1, *idbuf.shape[1:]), jnp.int32)

    @pl.when(here == n_ctx - 1)
    def _():
        rcv[...] = jnp.zeros(rcv.shape, BF)

    pl.semaphore_wait(barrier, 3 + has_next.astype(jnp.int32) + has_prev.astype(jnp.int32))

    def remote(src, dst, ssem, rsem, peer):
        return pltpu.make_async_remote_copy(
            src_ref=src, dst_ref=dst, send_sem=ssem, recv_sem=rsem,
            device_id=peer, device_id_type=MESH,
        )

    def kv_copy(hop, g, which):
        buf = kbuf if which == 0 else vbuf
        return [
            remote(buf.at[hop, g, r], buf.at[hop + 1, g, r], kv_s.at[hop, g, which, n],
                   kv_r.at[hop, g, which, n], {"ctx": nxt})
            for n, r in enumerate(pieces)
        ]

    def id_copy(hop):
        return remote(idbuf.at[hop], idbuf.at[hop + 1], id_s.at[hop], id_r.at[hop], {"ctx": nxt})

    def og_copy(i, src_slot, dst_slot, part, peer):
        return remote(ogbuf.at[src_slot, c, part], ogbuf.at[dst_slot, c, part],
                      x_s.at[i], x_r.at[i], {"mp": peer})

    started = []

    def go(cp, when=None):
        if when is None:
            cp.start()
        else:
            pl.when(when)(lambda: cp.start())
        started.append((cp, when))

    def arrive(cp, when):
        pl.when(when)(lambda: cp.wait_recv())

    def send_kv(hop, g, which):
        for n in range(PIECES):
            go(kv[hop, g, which][n], has_next)

    kv = {(hop, g, w): kv_copy(hop, g, w) for hop in range(3) for g in range(2) for w in range(2)}
    idc = [id_copy(hop) for hop in range(3)]
    everything = pl.ds(0, deep)
    og_own = og_copy(0, 0, 0, everything, partner)
    og_rt = og_copy(1, 0, 1, top, right)
    og_rb = og_copy(2, 0, 1, bot, right)
    og_lb = og_copy(3, 0, 3, bot, left)
    og_lt = og_copy(4, 0, 3, top, left)
    og_fr = og_copy(5, 1, 2, top, right)
    og_fl = og_copy(6, 3, 2, bot, left)
    share = {
        (1, 0): og_copy(7, 1, 1, top, partner),
        (1, 1): og_copy(8, 1, 1, bot, partner),
        (3, 0): og_copy(9, 3, 3, top, partner),
        (3, 1): og_copy(10, 3, 3, bot, partner),
        (2, 0): og_copy(11, 2, 2, top, partner),
        (2, 1): og_copy(12, 2, 2, bot, partner),
    }

    loads[("k", 0)].wait()
    send_kv(0, 0, 0)
    loads["og"].wait()
    go(og_rt)
    go(og_lb)
    go(og_rb)
    go(og_lt)
    go(og_own)
    loads[("v", 0)].wait()
    loads["ids"].wait()
    go(idc[0], has_next)
    send_kv(0, 0, 1)

    def forward(hop, g, which, n):
        arrive(kv[hop - 1, g, which][n], has_prev)
        if hop < 3:
            go(kv[hop, g, which][n], has_next)

    def spread_ids(hop):
        row = idbuf[hop]
        if hop:
            row = jnp.where(here >= hop, row, -1)
        kid[hop] = jnp.transpose(jnp.broadcast_to(row, (HEAD, rows)))

    def score(g, hop):
        keys = kbuf[hop, g]
        visible = jnp.concatenate([kid[hop]] * (rows // HEAD), axis=1) == jnp.broadcast_to(idbuf[0], (rows, rows))
        if hop == 0:
            visible = visible & (
                lax.broadcasted_iota(jnp.int32, (rows, rows), 0)
                <= lax.broadcasted_iota(jnp.int32, (rows, rows), 1)
            )
        for h in range(GROUP):
            i = g * GROUP + h
            t = jnp.tanh(lanes_dot(keys, q_v[:, i * HEAD:(i + 1) * HEAD]) * (SCALE / CAP))
            w = jnp.where(visible, jnp.exp(CAP * t), 0.0)
            wb[hop, i] = w
            cb[hop, i] = w * (SCALE - SCALE * (t * t))
            part = fold_rows(w)
            lacc[i] = part if hop == 0 else lacc[i] + part

    def attend(g, hop):
        vals = vbuf[hop, g]
        for h in range(GROUP):
            i = g * GROUP + h
            part = rows_dot(vals, wb[hop, i].astype(BF))
            att[i] = part if hop == 0 else att[i] + part

    def inverse(g):
        return [1.0 / jnp.sum(lacc[g * GROUP + h], axis=0, keepdims=True) for h in range(GROUP)]

    def deltas(g, inv):
        out = []
        for h in range(GROUP):
            i = g * GROUP + h
            d = do_v[i * HEAD:(i + 1) * HEAD, :].astype(F32)
            out.append(jnp.sum(d * att[i], axis=0, keepdims=True) * inv[h])
        return out

    def back_v(g, hop, inv):
        total = None
        for h in range(GROUP):
            i = g * GROUP + h
            probs = (wb[hop, i] * inv[h]).astype(BF)
            part = lanes_dot(probs, do_v[i * HEAD:(i + 1) * HEAD, :])
            total = part if total is None else total + part
        return total

    def back_k(g, hop, inv, delta):
        keys, vals = kbuf[hop, g], vbuf[hop, g]
        total = None
        for h in range(GROUP):
            i = g * GROUP + h
            grad = plain_dot(vals, do_v[i * HEAD:(i + 1) * HEAD, :])
            slope = ((cb[hop, i] * inv[h]) * (grad - delta[h])).astype(BF)
            part = plain_dot(slope, q_v[:, i * HEAD:(i + 1) * HEAD])
            total = part if total is None else total + part
            d = rows_dot(keys, slope)
            dqt[i] = d if hop == 3 else dqt[i] + d
        return total

    def back_copy(step, g, which):
        return [
            remote(snd.at[step, g, which, r], rcv.at[step, g, which, r],
                   b_s.at[step, g, which, n], b_r.at[step, g, which, n], {"ctx": prv})
            for n, r in enumerate(pieces)
        ]

    bc = {(s, g, w): back_copy(s, g, w) for s in range(3) for g in range(2) for w in range(2)}

    HEADS_A, HEADS_B = slice(0, GROUP * HEAD), slice(GROUP * HEAD, 2 * GROUP * HEAD)

    def project(rel, picked=slice(None)):
        at = pl.multiple_of(lax.rem(x + CHIPS - rel, CHIPS) * pair, HEAD)
        one = plain_dot(w_v[picked, pl.ds(at, pair)], ogbuf[rel].reshape(pair, rows))
        if rel == 0:
            gacc[picked] = one
        elif rel == 2:
            do_v[picked] = (gacc[picked] + one).astype(BF)
        else:
            gacc[picked] += one

    def pass_on(g, hop, which, n):
        step = 3 - hop
        r = slice(n * (rows // PIECES), (n + 1) * (rows // PIECES))
        value = part[hop, g, which, r, :]
        if step:
            arrive(bc[step - 1, g, which][n], has_next)
            value = value + rcv[step - 1, g, which, r, :].astype(F32)
        if hop:
            snd[step, g, which, r, :] = value.astype(BF)
            go(bc[step, g, which][n], has_prev)
        else:
            out = dk_ref if which == 0 else dv_ref
            out[r, g * HEAD:(g + 1) * HEAD] = value.astype(BF)

    def local_v(g, hop, inv):
        part[hop, g, 1] = back_v(g, hop, inv)

    def local_k(g, hop, inv, delta):
        part[hop, g, 0] = back_k(g, hop, inv, delta)

    def emit_q(g):
        for h in range(GROUP):
            i = g * GROUP + h
            dq_ref[:, i * HEAD:(i + 1) * HEAD] = jnp.transpose(dqt[i]).astype(BF)

    def ids_forward(hop):
        arrive(idc[hop - 1], has_prev)
        if hop < 3:
            go(idc[hop], has_next)
        spread_ids(hop)

    loads["q"].wait()
    loads["w"].wait()
    loads[("k", 1)].wait()
    loads[("v", 1)].wait()
    spread_ids(0)
    score(0, 0)
    attend(0, 0)
    score(1, 0)
    og_own.wait_recv()
    attend(1, 0)
    project(0)
    forward(1, 0, 0, 0)
    forward(1, 0, 0, 1)
    ids_forward(1)
    score(0, 1)
    forward(1, 0, 1, 0)
    forward(1, 0, 1, 1)
    send_kv(0, 1, 0)
    attend(0, 1)
    og_rt.wait_recv()
    go(og_fr)
    go(share[1, 0])
    og_lb.wait_recv()
    go(og_fl)
    go(share[3, 1])
    forward(2, 0, 0, 0)
    forward(2, 0, 0, 1)
    ids_forward(2)
    score(0, 2)
    forward(2, 0, 1, 0)
    forward(2, 0, 1, 1)
    send_kv(0, 1, 1)
    attend(0, 2)
    og_rb.wait_recv()
    go(share[1, 1])
    og_lt.wait_recv()
    go(share[3, 0])
    forward(1, 1, 0, 0)
    forward(1, 1, 0, 1)
    score(1, 1)
    share[1, 0].wait_recv()
    share[1, 1].wait_recv()
    project(1)
    forward(3, 0, 0, 0)
    share[3, 0].wait_recv()
    share[3, 1].wait_recv()
    project(3)
    forward(3, 0, 0, 1)
    ids_forward(3)
    score(0, 3)
    inv_a = inverse(0)
    og_fr.wait_recv()
    go(share[2, 0])
    og_fl.wait_recv()
    go(share[2, 1])
    forward(3, 0, 1, 0)
    forward(3, 0, 1, 1)
    attend(0, 3)
    share[2, 0].wait_recv()
    share[2, 1].wait_recv()
    project(2, HEADS_A)
    forward(1, 1, 1, 0)
    local_v(0, 3, inv_a)
    pass_on(0, 3, 1, 0)
    pass_on(0, 3, 1, 1)
    delta_a = deltas(0, inv_a)
    local_k(0, 3, inv_a, delta_a)
    forward(1, 1, 1, 1)
    pass_on(0, 3, 0, 0)
    pass_on(0, 3, 0, 1)
    local_v(0, 2, inv_a)
    local_k(0, 2, inv_a, delta_a)
    forward(2, 1, 0, 0)
    local_v(0, 1, inv_a)
    local_k(0, 1, inv_a, delta_a)
    project(2, HEADS_B)
    forward(2, 1, 0, 1)
    local_v(0, 0, inv_a)
    local_k(0, 0, inv_a, delta_a)
    score(1, 2)
    attend(1, 1)
    emit_q(0)
    forward(2, 1, 1, 0)
    pass_on(0, 2, 1, 0)
    forward(2, 1, 1, 1)
    attend(1, 2)
    pass_on(0, 2, 1, 1)
    forward(3, 1, 0, 0)
    pass_on(0, 2, 0, 0)
    forward(3, 1, 0, 1)
    score(1, 3)
    pass_on(0, 2, 0, 1)
    inv_b = inverse(1)
    local_v(1, 3, inv_b)
    pass_on(1, 3, 1, 0)
    pass_on(1, 3, 1, 1)
    local_v(1, 2, inv_b)
    local_v(1, 1, inv_b)
    local_v(1, 0, inv_b)
    forward(3, 1, 1, 0)
    pass_on(0, 1, 1, 0)
    forward(3, 1, 1, 1)
    attend(1, 3)
    delta_b = deltas(1, inv_b)
    local_k(1, 3, inv_b, delta_b)
    pass_on(1, 3, 0, 0)
    pass_on(1, 3, 0, 1)
    pass_on(0, 1, 1, 1)
    local_k(1, 2, inv_b, delta_b)
    local_k(1, 1, inv_b, delta_b)
    pass_on(0, 1, 0, 0)
    local_k(1, 0, inv_b, delta_b)
    emit_q(1)
    pass_on(0, 1, 0, 1)
    pass_on(1, 2, 1, 0)
    pass_on(1, 2, 1, 1)
    pass_on(0, 0, 1, 0)
    pass_on(1, 2, 0, 0)
    pass_on(1, 2, 0, 1)
    pass_on(0, 0, 1, 1)
    pass_on(0, 0, 0, 0)
    pass_on(0, 0, 0, 1)
    pass_on(1, 1, 1, 0)
    pass_on(1, 1, 1, 1)
    pass_on(1, 1, 0, 0)
    pass_on(1, 1, 0, 1)
    pass_on(1, 0, 1, 0)
    pass_on(1, 0, 1, 1)
    pass_on(1, 0, 0, 0)
    pass_on(1, 0, 0, 1)
    for cp, when in started:
        if when is None:
            cp.wait_send()
        else:
            pl.when(when)(functools.partial(cp.wait_send))


def settle(*refs):
    sems = refs[-1]
    n = len(refs) // 2
    copies = [pltpu.make_async_copy(refs[i], refs[n + i], sems.at[i]) for i in range(n)]
    for cp in copies:
        cp.start()
    for cp in copies:
        cp.wait()


def body(n_ctx, queries, keys, values, out_grad, doc_ids, w_out):
    rows = queries.shape[0]
    heads = queries.shape[1] // HEAD
    dma = pltpu.SemaphoreType.DMA
    anywhere = pl.BlockSpec(memory_space=pl.ANY)
    vmem = pl.BlockSpec(memory_space=pltpu.VMEM)
    shapes = (queries.shape, keys.shape, values.shape)
    grads = pl.pallas_call(
        functools.partial(kernel, n_ctx, rows),
        out_shape=tuple(pltpu.VMEM(sh, BF) for sh in shapes),
        in_specs=[anywhere] * 6,
        out_specs=(vmem, vmem, vmem),
        scratch_shapes=[
            pltpu.VMEM(queries.shape, BF),
            pltpu.VMEM((SPAN, 2, rows, HEAD), BF),
            pltpu.VMEM((SPAN, 2, rows, HEAD), BF),
            pltpu.VMEM((CHIPS, 2, out_grad.shape[1], rows), BF),
            pltpu.VMEM((SPAN, 1, rows), jnp.int32),
            pltpu.VMEM(w_out.shape, BF),
            pltpu.VMEM((heads * HEAD, rows), BF),
            pltpu.VMEM((SPAN, heads, rows, rows), F32),
            pltpu.VMEM((SPAN, heads, rows, rows), F32),
            pltpu.VMEM((heads, 8, rows), F32),
            pltpu.VMEM((heads, HEAD, rows), F32),
            pltpu.VMEM((heads, HEAD, rows), F32),
            pltpu.VMEM((heads * HEAD, rows), F32),
            pltpu.VMEM((SPAN, rows, HEAD), jnp.int32),
            pltpu.VMEM((SPAN, 2, 2, rows, HEAD), F32),
            pltpu.VMEM((3, 2, 2, rows, HEAD), BF),
            pltpu.VMEM((3, 2, 2, rows, HEAD), BF),
            dma((8,)),
            dma((3, 2, 2, PIECES)),
            dma((3, 2, 2, PIECES)),
            dma((3,)),
            dma((3,)),
            dma((13,)),
            dma((13,)),
            dma((3, 2, 2, PIECES)),
            dma((3, 2, 2, PIECES)),
        ],
        compiler_params=pltpu.CompilerParams(
            collective_id=0, has_side_effects=True, vmem_limit_bytes=60000 * 1024
        ),
    )(queries, keys, values, out_grad.T, doc_ids.reshape(1, rows), w_out)
    grads = [pltpu.with_memory_space_constraint(g, pltpu.VMEM) for g in grads]
    return pl.pallas_call(
        settle,
        out_shape=tuple(jax.ShapeDtypeStruct(sh, BF) for sh in shapes),
        in_specs=[vmem] * 3,
        out_specs=(anywhere,) * 3,
        scratch_shapes=[dma((3,))],
    )(*grads)


def solution(mesh):
    placed = (
        P("ctx", "mp"),
        P("ctx", "mp"),
        P("ctx", "mp"),
        P("ctx", "mp"),
        P("ctx"),
        P("mp", None),
    )
    return jax.shard_map(
        functools.partial(body, mesh.shape["ctx"]),
        mesh=mesh,
        in_specs=placed,
        out_specs=(P("ctx", "mp"), P("ctx", "mp"), P("ctx", "mp")),
        check_vma=False,
    )
```

```python
import functools
import jax
import jax.numpy as jnp
from jax import lax
from jax.experimental import pallas as pl
from jax.experimental.pallas import tpu as pltpu
from jax.sharding import PartitionSpec as P

HEAD = 128
SPAN = 4
GROUP = 2
CAP = 50.0
SCALE = 1.0 / 12.0
MESH = pl.DeviceIdType.MESH
BF = jnp.bfloat16
F32 = jnp.float32
CHIPS = 4
PIECES = 1


def lanes_dot(a, b):
    return lax.dot_general(a, b, (((1,), (1,)), ((), ())), preferred_element_type=F32)


def rows_dot(a, b):
    return lax.dot_general(a, b, (((0,), (0,)), ((), ())), preferred_element_type=F32)


def plain_dot(a, b):
    return lax.dot_general(a, b, (((1,), (0,)), ((), ())), preferred_element_type=F32)


def fold_rows(a):
    rows, cols = a.shape
    return jnp.sum(a.reshape(rows // 8, 8, cols), axis=0)


def kernel(
    n_ctx, rows,
    q_hbm, k_hbm, v_hbm, og_hbm, ids_hbm, w_hbm,
    dq_ref, dk_ref, dv_ref,
    q_v, kbuf, vbuf, ogbuf, idbuf, w_v, do_v,
    cb, wb, lacc, att, dqt, gacc, kid, part, snd, rcv,
    load_sem, kv_s, kv_r, id_s, id_r, x_s, x_r, b_s, b_r,
):
    here = lax.axis_index("ctx")
    m = lax.axis_index("mp")
    x = m // 2
    c = m % 2
    nxt = lax.rem(here + 1, n_ctx)
    prv = lax.rem(here + n_ctx - 1, n_ctx)
    partner = x * 2 + (1 - c)
    right = lax.rem(x + 1, CHIPS) * 2 + c
    left = lax.rem(x + CHIPS - 1, CHIPS) * 2 + c
    deep = ogbuf.shape[2]
    half = deep // 2
    top, bot = pl.ds(0, half), pl.ds(half, half)
    pair = w_hbm.shape[1] // CHIPS
    has_next = here < n_ctx - 1
    has_prev = here > 0
    pieces = [pl.ds(n * (rows // PIECES), rows // PIECES) for n in range(PIECES)]

    barrier = pltpu.get_barrier_semaphore()
    for peer in ({"mp": partner}, {"mp": right}, {"mp": left}):
        pl.semaphore_signal(barrier, inc=1, device_id=peer, device_id_type=MESH)

    @pl.when(has_next)
    def _():
        pl.semaphore_signal(barrier, inc=1, device_id={"ctx": nxt}, device_id_type=MESH)

    @pl.when(has_prev)
    def _():
        pl.semaphore_signal(barrier, inc=1, device_id={"ctx": prv}, device_id_type=MESH)

    loads = {}

    def load(name, src, dst):
        cp = pltpu.make_async_copy(src, dst, load_sem.at[len(loads)])
        cp.start()
        loads[name] = cp

    for g in range(2):
        cols = pl.ds(g * HEAD, HEAD)
        load(("k", g), k_hbm.at[:, cols], kbuf.at[0, g])
        load(("v", g), v_hbm.at[:, cols], vbuf.at[0, g])
        if g == 0:
            load("og", og_hbm, ogbuf.at[0, c])
            load("ids", ids_hbm, idbuf.at[0])
            load("q", q_hbm, q_v)
    load("w", w_hbm, w_v)

    @pl.when(here == 0)
    def _():
        kbuf[1:] = jnp.zeros((SPAN - 1, *kbuf.shape[1:]), BF)
        vbuf[1:] = jnp.zeros((SPAN - 1, *vbuf.shape[1:]), BF)
        idbuf[1:] = jnp.zeros((SPAN - 1, *idbuf.shape[1:]), jnp.int32)

    @pl.when(here == n_ctx - 1)
    def _():
        rcv[...] = jnp.zeros(rcv.shape, BF)

    pl.semaphore_wait(barrier, 3 + has_next.astype(jnp.int32) + has_prev.astype(jnp.int32))

    def remote(src, dst, ssem, rsem, peer):
        return pltpu.make_async_remote_copy(
            src_ref=src, dst_ref=dst, send_sem=ssem, recv_sem=rsem,
            device_id=peer, device_id_type=MESH,
        )

    def kv_copy(hop, g, which):
        buf = kbuf if which == 0 else vbuf
        return [
            remote(buf.at[hop, g, r], buf.at[hop + 1, g, r], kv_s.at[hop, g, which, n],
                   kv_r.at[hop, g, which, n], {"ctx": nxt})
            for n, r in enumerate(pieces)
        ]

    def id_copy(hop):
        return remote(idbuf.at[hop], idbuf.at[hop + 1], id_s.at[hop], id_r.at[hop], {"ctx": nxt})

    def og_copy(i, src_slot, dst_slot, part, peer):
        return remote(ogbuf.at[src_slot, c, part], ogbuf.at[dst_slot, c, part],
                      x_s.at[i], x_r.at[i], {"mp": peer})

    started = []

    def go(cp, when=None):
        if when is None:
            cp.start()
        else:
            pl.when(when)(lambda: cp.start())
        started.append((cp, when))

    def arrive(cp, when):
        pl.when(when)(lambda: cp.wait_recv())

    def send_kv(hop, g, which):
        for n in range(PIECES):
            go(kv[hop, g, which][n], has_next)

    kv = {(hop, g, w): kv_copy(hop, g, w) for hop in range(3) for g in range(2) for w in range(2)}
    idc = [id_copy(hop) for hop in range(3)]
    everything = pl.ds(0, deep)
    og_own = og_copy(0, 0, 0, everything, partner)
    og_rt = og_copy(1, 0, 1, top, right)
    og_rb = og_copy(2, 0, 1, bot, right)
    og_lb = og_copy(3, 0, 3, bot, left)
    og_lt = og_copy(4, 0, 3, top, left)
    og_fr = og_copy(5, 1, 2, top, right)
    og_fl = og_copy(6, 3, 2, bot, left)
    share = {
        (1, 0): og_copy(7, 1, 1, top, partner),
        (1, 1): og_copy(8, 1, 1, bot, partner),
        (3, 0): og_copy(9, 3, 3, top, partner),
        (3, 1): og_copy(10, 3, 3, bot, partner),
        (2, 0): og_copy(11, 2, 2, top, partner),
        (2, 1): og_copy(12, 2, 2, bot, partner),
    }

    loads[("k", 0)].wait()
    send_kv(0, 0, 0)
    loads["og"].wait()
    go(og_rt)
    go(og_lb)
    go(og_rb)
    go(og_lt)
    go(og_own)
    loads[("v", 0)].wait()
    loads["ids"].wait()
    go(idc[0], has_next)
    send_kv(0, 0, 1)

    def forward(hop, g, which, n):
        arrive(kv[hop - 1, g, which][n], has_prev)
        if hop < 3:
            go(kv[hop, g, which][n], has_next)

    def spread_ids(hop):
        row = idbuf[hop]
        if hop:
            row = jnp.where(here >= hop, row, -1)
        kid[hop] = jnp.transpose(jnp.broadcast_to(row, (HEAD, rows)))

    def score(g, hop):
        keys = kbuf[hop, g]
        visible = jnp.concatenate([kid[hop]] * (rows // HEAD), axis=1) == jnp.broadcast_to(idbuf[0], (rows, rows))
        if hop == 0:
            visible = visible & (
                lax.broadcasted_iota(jnp.int32, (rows, rows), 0)
                <= lax.broadcasted_iota(jnp.int32, (rows, rows), 1)
            )
        for h in range(GROUP):
            i = g * GROUP + h
            t = jnp.tanh(lanes_dot(keys, q_v[:, i * HEAD:(i + 1) * HEAD]) * (SCALE / CAP))
            w = jnp.where(visible, jnp.exp(CAP * t), 0.0)
            wb[hop, i] = w
            cb[hop, i] = w * (SCALE - SCALE * (t * t))
            part = fold_rows(w)
            lacc[i] = part if hop == 0 else lacc[i] + part

    def attend(g, hop):
        vals = vbuf[hop, g]
        for h in range(GROUP):
            i = g * GROUP + h
            part = rows_dot(vals, wb[hop, i].astype(BF))
            att[i] = part if hop == 0 else att[i] + part

    def inverse(g):
        return [1.0 / jnp.sum(lacc[g * GROUP + h], axis=0, keepdims=True) for h in range(GROUP)]

    def deltas(g, inv):
        out = []
        for h in range(GROUP):
            i = g * GROUP + h
            d = do_v[i * HEAD:(i + 1) * HEAD, :].astype(F32)
            out.append(jnp.sum(d * att[i], axis=0, keepdims=True) * inv[h])
        return out

    def back_v(g, hop, inv):
        total = None
        for h in range(GROUP):
            i = g * GROUP + h
            probs = (wb[hop, i] * inv[h]).astype(BF)
            part = lanes_dot(probs, do_v[i * HEAD:(i + 1) * HEAD, :])
            total = part if total is None else total + part
        return total

    def back_k(g, hop, inv, delta):
        keys, vals = kbuf[hop, g], vbuf[hop, g]
        total = None
        for h in range(GROUP):
            i = g * GROUP + h
            grad = plain_dot(vals, do_v[i * HEAD:(i + 1) * HEAD, :])
            slope = ((cb[hop, i] * inv[h]) * (grad - delta[h])).astype(BF)
            part = plain_dot(slope, q_v[:, i * HEAD:(i + 1) * HEAD])
            total = part if total is None else total + part
            d = rows_dot(keys, slope)
            dqt[i] = d if hop == 3 else dqt[i] + d
        return total

    def back_copy(step, g, which):
        return [
            remote(snd.at[step, g, which, r], rcv.at[step, g, which, r],
                   b_s.at[step, g, which, n], b_r.at[step, g, which, n], {"ctx": prv})
            for n, r in enumerate(pieces)
        ]

    bc = {(s, g, w): back_copy(s, g, w) for s in range(3) for g in range(2) for w in range(2)}

    HEADS_A, HEADS_B = slice(0, GROUP * HEAD), slice(GROUP * HEAD, 2 * GROUP * HEAD)

    def project(rel, picked=slice(None)):
        at = pl.multiple_of(lax.rem(x + CHIPS - rel, CHIPS) * pair, HEAD)
        one = plain_dot(w_v[picked, pl.ds(at, pair)], ogbuf[rel].reshape(pair, rows))
        if rel == 0:
            gacc[picked] = one
        elif rel == 2:
            do_v[picked] = (gacc[picked] + one).astype(BF)
        else:
            gacc[picked] += one

    def pass_on(g, hop, which, n):
        step = 3 - hop
        r = slice(n * (rows // PIECES), (n + 1) * (rows // PIECES))
        value = part[hop, g, which, r, :]
        if step:
            arrive(bc[step - 1, g, which][n], has_next)
            value = value + rcv[step - 1, g, which, r, :].astype(F32)
        if hop:
            snd[step, g, which, r, :] = value.astype(BF)
            go(bc[step, g, which][n], has_prev)
        else:
            out = dk_ref if which == 0 else dv_ref
            out[r, g * HEAD:(g + 1) * HEAD] = value.astype(BF)

    def local_v(g, hop, inv):
        part[hop, g, 1] = back_v(g, hop, inv)

    def local_k(g, hop, inv, delta):
        part[hop, g, 0] = back_k(g, hop, inv, delta)

    def emit_q(g):
        for h in range(GROUP):
            i = g * GROUP + h
            dq_ref[:, i * HEAD:(i + 1) * HEAD] = jnp.transpose(dqt[i]).astype(BF)

    def ids_forward(hop):
        arrive(idc[hop - 1], has_prev)
        if hop < 3:
            go(idc[hop], has_next)
        spread_ids(hop)

    loads["q"].wait()
    loads["w"].wait()
    loads[("k", 1)].wait()
    loads[("v", 1)].wait()
    spread_ids(0)
    score(0, 0)
    attend(0, 0)
    og_own.wait_recv()
    score(1, 0)
    attend(1, 0)
    project(0)
    forward(1, 0, 0, 0)
    ids_forward(1)
    score(0, 1)
    forward(1, 0, 1, 0)
    send_kv(0, 1, 0)
    attend(0, 1)
    og_rt.wait_recv()
    go(og_fr)
    go(share[1, 0])
    og_lb.wait_recv()
    go(og_fl)
    go(share[3, 1])
    forward(2, 0, 0, 0)
    ids_forward(2)
    score(0, 2)
    og_rb.wait_recv()
    go(share[1, 1])
    og_lt.wait_recv()
    go(share[3, 0])
    forward(2, 0, 1, 0)
    send_kv(0, 1, 1)
    attend(0, 2)
    share[1, 0].wait_recv()
    share[1, 1].wait_recv()
    project(1)
    forward(1, 1, 0, 0)
    share[3, 0].wait_recv()
    share[3, 1].wait_recv()
    project(3)
    score(1, 1)
    og_fr.wait_recv()
    go(share[2, 0])
    og_fl.wait_recv()
    go(share[2, 1])
    forward(3, 0, 0, 0)
    ids_forward(3)
    score(0, 3)
    inv_a = inverse(0)
    share[2, 0].wait_recv()
    share[2, 1].wait_recv()
    project(2, HEADS_A)
    forward(3, 0, 1, 0)
    local_v(0, 3, inv_a)
    pass_on(0, 3, 1, 0)
    local_v(0, 2, inv_a)
    attend(0, 3)
    delta_a = deltas(0, inv_a)
    local_k(0, 3, inv_a, delta_a)
    pass_on(0, 3, 0, 0)
    forward(1, 1, 1, 0)
    local_k(0, 2, inv_a, delta_a)
    local_v(0, 1, inv_a)
    local_k(0, 1, inv_a, delta_a)
    project(2, HEADS_B)
    forward(2, 1, 0, 0)
    local_v(0, 0, inv_a)
    local_k(0, 0, inv_a, delta_a)
    score(1, 2)
    attend(1, 1)
    emit_q(0)
    pass_on(0, 2, 1, 0)
    forward(2, 1, 1, 0)
    attend(1, 2)
    pass_on(0, 2, 0, 0)
    forward(3, 1, 0, 0)
    score(1, 3)
    inv_b = inverse(1)
    local_v(1, 3, inv_b)
    pass_on(1, 3, 1, 0)
    local_v(1, 2, inv_b)
    local_v(1, 1, inv_b)
    local_v(1, 0, inv_b)
    pass_on(0, 1, 1, 0)
    forward(3, 1, 1, 0)
    attend(1, 3)
    delta_b = deltas(1, inv_b)
    local_k(1, 3, inv_b, delta_b)
    pass_on(1, 3, 0, 0)
    pass_on(0, 1, 0, 0)
    local_k(1, 2, inv_b, delta_b)
    local_k(1, 1, inv_b, delta_b)
    local_k(1, 0, inv_b, delta_b)
    emit_q(1)
    pass_on(1, 2, 1, 0)
    pass_on(0, 0, 1, 0)
    pass_on(1, 2, 0, 0)
    pass_on(0, 0, 0, 0)
    pass_on(1, 1, 1, 0)
    pass_on(1, 1, 0, 0)
    pass_on(1, 0, 1, 0)
    pass_on(1, 0, 0, 0)
    for cp, when in started:
        if when is None:
            cp.wait_send()
        else:
            pl.when(when)(functools.partial(cp.wait_send))


def settle(*refs):
    sems = refs[-1]
    n = len(refs) // 2
    copies = [pltpu.make_async_copy(refs[i], refs[n + i], sems.at[i]) for i in range(n)]
    for cp in copies:
        cp.start()
    for cp in copies:
        cp.wait()


def body(n_ctx, queries, keys, values, out_grad, doc_ids, w_out):
    rows = queries.shape[0]
    heads = queries.shape[1] // HEAD
    dma = pltpu.SemaphoreType.DMA
    anywhere = pl.BlockSpec(memory_space=pl.ANY)
    vmem = pl.BlockSpec(memory_space=pltpu.VMEM)
    shapes = (queries.shape, keys.shape, values.shape)
    grads = pl.pallas_call(
        functools.partial(kernel, n_ctx, rows),
        out_shape=tuple(pltpu.VMEM(sh, BF) for sh in shapes),
        in_specs=[anywhere] * 6,
        out_specs=(vmem, vmem, vmem),
        scratch_shapes=[
            pltpu.VMEM(queries.shape, BF),
            pltpu.VMEM((SPAN, 2, rows, HEAD), BF),
            pltpu.VMEM((SPAN, 2, rows, HEAD), BF),
            pltpu.VMEM((CHIPS, 2, out_grad.shape[1], rows), BF),
            pltpu.VMEM((SPAN, 1, rows), jnp.int32),
            pltpu.VMEM(w_out.shape, BF),
            pltpu.VMEM((heads * HEAD, rows), BF),
            pltpu.VMEM((SPAN, heads, rows, rows), F32),
            pltpu.VMEM((SPAN, heads, rows, rows), F32),
            pltpu.VMEM((heads, 8, rows), F32),
            pltpu.VMEM((heads, HEAD, rows), F32),
            pltpu.VMEM((heads, HEAD, rows), F32),
            pltpu.VMEM((heads * HEAD, rows), F32),
            pltpu.VMEM((SPAN, rows, HEAD), jnp.int32),
            pltpu.VMEM((SPAN, 2, 2, rows, HEAD), F32),
            pltpu.VMEM((3, 2, 2, rows, HEAD), BF),
            pltpu.VMEM((3, 2, 2, rows, HEAD), BF),
            dma((8,)),
            dma((3, 2, 2, PIECES)),
            dma((3, 2, 2, PIECES)),
            dma((3,)),
            dma((3,)),
            dma((13,)),
            dma((13,)),
            dma((3, 2, 2, PIECES)),
            dma((3, 2, 2, PIECES)),
        ],
        compiler_params=pltpu.CompilerParams(
            collective_id=0, has_side_effects=True, vmem_limit_bytes=60000 * 1024
        ),
    )(queries, keys, values, out_grad.T, doc_ids.reshape(1, rows), w_out)
    grads = [pltpu.with_memory_space_constraint(g, pltpu.VMEM) for g in grads]
    return pl.pallas_call(
        settle,
        out_shape=tuple(jax.ShapeDtypeStruct(sh, BF) for sh in shapes),
        in_specs=[vmem] * 3,
        out_specs=(anywhere,) * 3,
        scratch_shapes=[dma((3,))],
    )(*grads)


def solution(mesh):
    placed = (
        P("ctx", "mp"),
        P("ctx", "mp"),
        P("ctx", "mp"),
        P("ctx", "mp"),
        P("ctx"),
        P("mp", None),
    )
    return jax.shard_map(
        functools.partial(body, mesh.shape["ctx"]),
        mesh=mesh,
        in_specs=placed,
        out_specs=(P("ctx", "mp"), P("ctx", "mp"), P("ctx", "mp")),
        check_vma=False,
    )
```
